32 devices in a mesh: ep: 32 (over z, y, x, core).
Axes of the slice: x: 2, y: 2, z: 4, core: 2. Of those that a mesh axis runs over, the one named last changes fastest.
Arguments:
- x_tokens: bfloat16 [32768, 1536], P('ep')
- w_router: bfloat16 [1536, 64], replicated
- w_gate: bfloat16 [64, 1536, 512], P('ep')
- w_up: bfloat16 [64, 1536, 512], P('ep')
- w_down: bfloat16 [64, 512, 1536], P('ep')
- topk_idx: int32 [32768, 6], P('ep')
- dy_tokens: bfloat16 [32768, 1536], P('ep')
Outputs:
- output 1: bfloat16 [32768, 1536], P('ep')
- output 2: float32 [], replicated
- output 3: bfloat16 [32768, 1536], P('ep')
- output 4: float32 [1536, 64], replicated
- output 5: float32 [64, 1536, 512], P('ep')
- output 6: float32 [64, 1536, 512], P('ep')
- output 7: float32 [64, 512, 1536], P('ep')
All inputs are finite; a program needn't handle non-finite values.
Results may differ from the reference program's by a relative error of at most 0.00525984.
Values are sent between devices in bfloat16 or wider.
A program may use at most 1 GiB of HBM per device.

```python
import jax
import jax.numpy as jnp
from jax import lax

MODEL_DIM = 1536
FF_DIM = 512
NUM_EXPERTS = 64
TOP_K = 6
TOK_PER_DEV = 1024
NUM_DEVICES = 32
ALL_TOKENS = NUM_DEVICES * TOK_PER_DEV
CAPACITY = (5 * TOK_PER_DEV * TOP_K + 4 * NUM_EXPERTS - 1) // (4 * NUM_EXPERTS)
AUX_COEF = 0.001


def draw_routing(key):
    bias_key, score_key = jax.random.split(key)
    dev_bias = jax.random.randint(bias_key, (NUM_DEVICES, 1, NUM_EXPERTS), 0, 61)
    scores = jax.random.randint(score_key, (NUM_DEVICES, TOK_PER_DEV, NUM_EXPERTS), 0, 1000)
    ranked = (scores + dev_bias) * NUM_EXPERTS + jnp.arange(NUM_EXPERTS, dtype=jnp.int32)
    chosen = lax.top_k(ranked, TOP_K)[1]
    return chosen.reshape(ALL_TOKENS, TOP_K).astype(jnp.int32)


def setup_inputs(seed: int = 0) -> dict:
    key_list = jax.random.split(jax.random.key(seed), 7)
    topk_idx = draw_routing(key_list[0])
    router_f = jax.random.normal(key_list[1], (MODEL_DIM, NUM_EXPERTS), jnp.float32) * MODEL_DIM ** -0.5
    chosen_hot = jnp.zeros((ALL_TOKENS, NUM_EXPERTS), jnp.float32).at[jnp.arange(ALL_TOKENS)[:, None], topk_idx].set(1.0)
    x_noise = jax.random.normal(key_list[2], (ALL_TOKENS, MODEL_DIM), jnp.float32)
    x_tokens = x_noise + 3.0 * jnp.dot(chosen_hot, router_f.T)
    w_gate = jax.random.normal(key_list[3], (NUM_EXPERTS, MODEL_DIM, FF_DIM), jnp.float32) * MODEL_DIM ** -0.5
    w_up = jax.random.normal(key_list[4], (NUM_EXPERTS, MODEL_DIM, FF_DIM), jnp.float32) * MODEL_DIM ** -0.5
    w_down = jax.random.normal(key_list[5], (NUM_EXPERTS, FF_DIM, MODEL_DIM), jnp.float32) * FF_DIM ** -0.5
    dy_tokens = jax.random.normal(key_list[6], (ALL_TOKENS, MODEL_DIM), jnp.float32)
    return {
        "x_tokens": x_tokens.astype(jnp.bfloat16),
        "w_router": router_f.astype(jnp.bfloat16),
        "w_gate": w_gate.astype(jnp.bfloat16),
        "w_up": w_up.astype(jnp.bfloat16),
        "w_down": w_down.astype(jnp.bfloat16),
        "topk_idx": topk_idx,
        "dy_tokens": dy_tokens.astype(jnp.bfloat16),
    }


def reference(x_tokens, w_router, w_gate, w_up, w_down, topk_idx, dy_tokens):
    logits = jnp.dot(x_tokens, w_router, preferred_element_type=jnp.float32)
    router_prob = jax.nn.softmax(logits, axis=-1)
    counts = jax.ops.segment_sum(jnp.ones((ALL_TOKENS * TOP_K,), jnp.float32), topk_idx.reshape(-1), num_segments=NUM_EXPERTS)
    load_frac = counts / (ALL_TOKENS * TOP_K)
    mean_prob = jnp.mean(router_prob, axis=0)
    aux_loss = AUX_COEF * NUM_EXPERTS * jnp.sum(load_frac * mean_prob)
    aux_grad = AUX_COEF * NUM_EXPERTS * load_frac / ALL_TOKENS
    w_gate32 = w_gate.astype(jnp.float32)
    w_up32 = w_up.astype(jnp.float32)
    w_down32 = w_down.astype(jnp.float32)
    zero_row = jnp.zeros((1, MODEL_DIM), x_tokens.dtype)
    n_slots = NUM_EXPERTS * CAPACITY

    def device_step(carry_acc, dev_in):
        dwg_acc, dwu_acc, dwd_acc, dwr_acc = carry_acc
        x_dev, prob_dev, idx_dev, dy_dev = dev_in
        pick_prob = jnp.take_along_axis(prob_dev, idx_dev, axis=1)
        pick_sum = jnp.sum(pick_prob, axis=1, keepdims=True)
        gate_f32 = pick_prob / pick_sum
        gate_bf = gate_f32.astype(jnp.bfloat16)
        choice_mask = idx_dev[:, :, None] == jnp.arange(NUM_EXPERTS)[None, None, :]
        expert_hot = jnp.sum(choice_mask.astype(jnp.int32), axis=1)
        earlier = jnp.cumsum(expert_hot, axis=0) - expert_hot
        position = jnp.take_along_axis(earlier, idx_dev, axis=1)
        slot_ids = jnp.where(position < CAPACITY, idx_dev * CAPACITY + position, n_slots)
        flat_slots = slot_ids.reshape(-1)
        x_rep = jnp.broadcast_to(x_dev[:, None, :], (TOK_PER_DEV, TOP_K, MODEL_DIM)).reshape(TOK_PER_DEV * TOP_K, MODEL_DIM)
        buf_x = jnp.zeros((n_slots + 1, MODEL_DIM), x_dev.dtype).at[flat_slots].set(x_rep)[:n_slots]
        buf_x32 = buf_x.reshape(NUM_EXPERTS, CAPACITY, MODEL_DIM).astype(jnp.float32)
        gate_pre = jnp.einsum("ecd,edf->ecf", buf_x32, w_gate32)
        up_pre = jnp.einsum("ecd,edf->ecf", buf_x32, w_up32)
        act_gate = jax.nn.silu(gate_pre)
        hidden = (act_gate * up_pre).astype(jnp.bfloat16).astype(jnp.float32)
        out_slot = jnp.einsum("ecf,efd->ecd", hidden, w_down32).astype(jnp.bfloat16)
        out_tok = jnp.concatenate([out_slot.reshape(n_slots, MODEL_DIM), zero_row])[slot_ids]
        y_dev = jnp.sum(gate_bf.astype(jnp.float32)[:, :, None] * out_tok.astype(jnp.float32), axis=1).astype(jnp.bfloat16)
        do_tok = (gate_bf.astype(jnp.float32)[:, :, None] * dy_dev.astype(jnp.float32)[:, None, :]).astype(jnp.bfloat16)
        buf_do = jnp.zeros((n_slots + 1, MODEL_DIM), dy_dev.dtype).at[flat_slots].set(do_tok.reshape(TOK_PER_DEV * TOP_K, MODEL_DIM))[:n_slots]
        buf_do32 = buf_do.reshape(NUM_EXPERTS, CAPACITY, MODEL_DIM).astype(jnp.float32)
        dwd_new = dwd_acc + jnp.einsum("ecf,ecd->efd", hidden, buf_do32)
        d_hidden = jnp.einsum("ecd,efd->ecf", buf_do32, w_down32).astype(jnp.bfloat16).astype(jnp.float32)
        sigmoid_g = jax.nn.sigmoid(gate_pre)
        d_gate_pre = (d_hidden * up_pre * sigmoid_g * (1.0 + gate_pre * (1.0 - sigmoid_g))).astype(jnp.bfloat16).astype(jnp.float32)
        d_up_pre = (d_hidden * act_gate).astype(jnp.bfloat16).astype(jnp.float32)
        dwg_new = dwg_acc + jnp.einsum("ecd,ecf->edf", buf_x32, d_gate_pre)
        dwu_new = dwu_acc + jnp.einsum("ecd,ecf->edf", buf_x32, d_up_pre)
        dx_slot = (jnp.einsum("ecf,edf->ecd", d_gate_pre, w_gate32) + jnp.einsum("ecf,edf->ecd", d_up_pre, w_up32)).astype(jnp.bfloat16)
        dx_tok = jnp.concatenate([dx_slot.reshape(n_slots, MODEL_DIM), zero_row])[slot_ids]
        dx_expert = jnp.sum(dx_tok.astype(jnp.float32), axis=1)
        d_gate = jnp.sum(out_tok.astype(jnp.float32) * dy_dev.astype(jnp.float32)[:, None, :], axis=2)
        d_pick = (d_gate - jnp.sum(d_gate * gate_f32, axis=1, keepdims=True)) / pick_sum
        d_prob = jnp.sum(jnp.where(choice_mask, d_pick[:, :, None], 0.0), axis=1) + aux_grad
        d_logit = prob_dev * (d_prob - jnp.sum(prob_dev * d_prob, axis=1, keepdims=True))
        d_logit_bf = d_logit.astype(jnp.bfloat16)
        dwr_new = dwr_acc + jnp.dot(x_dev.T, d_logit_bf, preferred_element_type=jnp.float32)
        dx_dev = (dx_expert + jnp.dot(d_logit_bf, w_router.T, preferred_element_type=jnp.float32)).astype(jnp.bfloat16)
        return (dwg_new, dwu_new, dwd_new, dwr_new), (y_dev, dx_dev)

    init_acc = (
        jnp.zeros((NUM_EXPERTS, MODEL_DIM, FF_DIM), jnp.float32),
        jnp.zeros((NUM_EXPERTS, MODEL_DIM, FF_DIM), jnp.float32),
        jnp.zeros((NUM_EXPERTS, FF_DIM, MODEL_DIM), jnp.float32),
        jnp.zeros((MODEL_DIM, NUM_EXPERTS), jnp.float32),
    )
    dev_inputs = (
        x_tokens.reshape(NUM_DEVICES, TOK_PER_DEV, MODEL_DIM),
        router_prob.reshape(NUM_DEVICES, TOK_PER_DEV, NUM_EXPERTS),
        topk_idx.reshape(NUM_DEVICES, TOK_PER_DEV, TOP_K),
        dy_tokens.reshape(NUM_DEVICES, TOK_PER_DEV, MODEL_DIM),
    )
    final_acc, dev_outs = lax.scan(device_step, init_acc, dev_inputs)
    y_tokens = dev_outs[0].reshape(ALL_TOKENS, MODEL_DIM)
    dx_tokens = dev_outs[1].reshape(ALL_TOKENS, MODEL_DIM)
    return (y_tokens, aux_loss, dx_tokens, final_acc[3], final_acc[0], final_acc[1], final_acc[2])
```

```python
import functools

import jax
import jax.numpy as jnp
from jax import lax
from jax.experimental import pallas as pl
from jax.experimental.pallas import tpu as pltpu
from jax.sharding import PartitionSpec as P

AUX_COEF = 0.001
N_PLANE = 8
X_PIECES = 2
Y_PIECES = 2
DX_PIECES = 4
F32 = jnp.float32
BF16 = jnp.bfloat16


def one_hot_rows(pos, capacity):
    n, _, tok = pos.shape
    slot = lax.broadcasted_iota(jnp.int32, (n, capacity, tok), 1).astype(F32)
    return slot == pos


def dispatch_kernel(capacity, weighted, pos_ref, wt_ref, x_ref, out0_ref, out1_ref):
    n_dst = pos_ref.shape[2]
    tok = x_ref.shape[1]
    for g, out_ref in enumerate((out0_ref, out1_ref)):
        mask = one_hot_rows(pos_ref[0, g], capacity)
        value = jnp.broadcast_to(wt_ref[0, g], mask.shape) if weighted else jnp.ones(mask.shape, F32)
        sel = jnp.where(mask, value, 0.0).reshape(n_dst * capacity, tok).astype(BF16)
        rows = jnp.dot(sel, x_ref[0], preferred_element_type=F32)
        out_ref[:, 0] = rows.reshape(n_dst, capacity, rows.shape[1]).astype(BF16)


def dispatch(pos, wt, x_line, capacity, weighted):
    n_src, _, n_dst, _, tok = pos.shape
    dim = x_line.shape[2]
    out = jax.ShapeDtypeStruct((n_dst, n_src, capacity, dim), BF16)
    table = pl.BlockSpec((1, 2, n_dst, 1, tok), lambda j: (j, 0, 0, 0, 0))
    out_spec = pl.BlockSpec((n_dst, 1, capacity, dim), lambda j: (0, j, 0, 0))
    return pl.pallas_call(
        functools.partial(dispatch_kernel, capacity, weighted),
        grid=(n_src,),
        in_specs=[table, table, pl.BlockSpec((1, tok, dim), lambda j: (j, 0, 0))],
        out_specs=[out_spec, out_spec],
        out_shape=[out, out],
        compiler_params=pltpu.CompilerParams(vmem_limit_bytes=60 * 2**20),
        cost_estimate=pl.CostEstimate(flops=4 * n_src * n_dst * capacity * tok * dim, bytes_accessed=36 * 2**20, transcendentals=0),
    )(pos, wt, x_line)


def combine_kernel(capacity, weighted, with_dot, pos_ref, wt_ref, rows0_ref, rows1_ref, *refs):
    dy_ref, acc_ref, a_ref = refs if with_dot else (None, refs[0], None)
    n, _, tok = pos_ref.shape[2:]
    for g, rows_ref in enumerate((rows0_ref, rows1_ref)):
        mask = one_hot_rows(pos_ref[0, g], capacity)
        value = jnp.broadcast_to(wt_ref[0, g], mask.shape) if weighted else jnp.ones(mask.shape, F32)
        sel = jnp.where(mask, value, 0.0).reshape(n * capacity, tok).astype(BF16)
        rows = rows_ref[:, 0].astype(F32).reshape(n * capacity, rows_ref.shape[3]).astype(BF16)
        part = lax.dot_general(sel, rows, (((0,), (0,)), ((), ())), preferred_element_type=F32)
        if g == 0:
            acc_ref[0] = part
        else:
            acc_ref[0] += part
        if with_dot:
            prod = lax.dot_general(rows, dy_ref[0], (((1,), (1,)), ((), ())), preferred_element_type=F32)
            prod = jnp.where(mask, prod.reshape(n, capacity, tok), 0.0)
            a_ref[0, g] = jnp.sum(prod, axis=1)


def combine(pos, wt, rows0, rows1, dy_line, piece, capacity, weighted):
    n_src, _, n_dst, _, tok = pos.shape
    dim = rows0.shape[3]
    table = pl.BlockSpec((1, 2, n_dst, 1, tok), lambda j: (j, 0, 0, 0, 0))
    rows_spec = pl.BlockSpec((n_dst, 1, capacity, dim), lambda j: (0, j, 0, 0))
    by_src = pl.BlockSpec((1, tok, dim), lambda j: (j, 0, 0))
    in_specs = [table, table, rows_spec, rows_spec]
    operands = [pos, wt, rows0, rows1]
    out_shape = [jax.ShapeDtypeStruct((n_src, tok, dim), F32)]
    out_specs = [by_src]
    with_dot = dy_line is not None
    if with_dot:
        in_specs.append(pl.BlockSpec((1, tok, dim), lambda j: (j, 0, piece)))
        operands.append(dy_line)
        out_shape.append(jax.ShapeDtypeStruct((n_src, 2, n_dst, tok), F32))
        out_specs.append(pl.BlockSpec((1, 2, n_dst, tok), lambda j: (j, 0, 0, 0)))
    flops = 4 * n_src * n_dst * capacity * tok * dim * (2 if with_dot else 1)
    return pl.pallas_call(
        functools.partial(combine_kernel, capacity, weighted, with_dot),
        grid=(n_src,),
        in_specs=in_specs,
        out_specs=out_specs,
        out_shape=out_shape,
        compiler_params=pltpu.CompilerParams(vmem_limit_bytes=63 * 2**20),
        cost_estimate=pl.CostEstimate(flops=flops, bytes_accessed=50 * 2**20, transcendentals=0),
    )(*operands)


def solution(mesh):
    n_dev = mesh.shape["ep"]
    n_line = n_dev // N_PLANE
    lines = [[z * N_PLANE + i for z in range(n_line)] for i in range(N_PLANE)]
    planes = [[z * N_PLANE + i for i in range(N_PLANE)] for z in range(n_line)]

    def local_block(x_loc, w_router, wg_loc, wu_loc, wd_loc, idx_loc, dy_loc):
        tok, dim = x_loc.shape
        top_k = idx_loc.shape[1]
        n_exp = w_router.shape[1]
        loc_exp = wg_loc.shape[0]
        capacity = (5 * tok * top_k + 4 * n_exp - 1) // (4 * n_exp)
        n_total = tok * n_dev
        me = lax.axis_index("ep")

        def columns(pieces):
            return [slice(i * dim // pieces, (i + 1) * dim // pieces) for i in range(pieces)]

        def after(value, earlier_value):
            return lax.optimization_barrier((value, earlier_value))[0]

        x_line = []
        for cols in columns(X_PIECES):
            part = x_loc[:, cols] if not x_line else after(x_loc[:, cols], x_line[-1])
            x_line.append(lax.all_gather(part, "ep", axis_index_groups=lines))
        dy_line = lax.all_gather(after(dy_loc, x_line[-1]), "ep", axis_index_groups=lines)

        logits = lax.dot_general(w_router, x_loc, (((0,), (1,)), ((), ())), preferred_element_type=F32)
        prob = jax.nn.softmax(logits, axis=0)
        idx_t = idx_loc.T
        hot = jnp.any(idx_t[:, None, :] == jnp.arange(n_exp, dtype=jnp.int32)[None, :, None], axis=0)
        hot_f = hot.astype(F32)
        before = (jnp.arange(tok)[:, None] < jnp.arange(tok)[None, :]).astype(BF16)
        earlier = jnp.dot(hot.astype(BF16), before, preferred_element_type=F32)
        pick_sum = jnp.sum(jnp.where(hot, prob, 0.0), axis=0, keepdims=True)
        gate = jnp.where(hot, prob, 0.0) / pick_sum
        gate_bf = gate.astype(BF16)
        kept = hot & (earlier < capacity)
        pos = jnp.where(kept, earlier, -1.0)

        count = jnp.sum(hot_f, axis=1)
        load = lax.psum(jnp.concatenate([count, jnp.sum(prob, axis=1)]), "ep")
        load_frac = load[:n_exp] / (n_total * top_k)
        mean_prob = load[n_exp:] / n_total
        aux_loss = AUX_COEF * n_exp * jnp.sum(load_frac * mean_prob)

        tables = jnp.stack([pos.astype(BF16), gate_bf]).reshape(2, n_line, N_PLANE, loc_exp, tok)
        tables = lax.all_to_all(after(tables.transpose(1, 0, 3, 2, 4), load), "ep", 0, 0, axis_index_groups=lines)
        tables = tables.astype(F32)[:, :, :, :, None, :]
        pos_line, gate_line = tables[:, 0], tables[:, 1]

        done = []

        def in_plane(rows, then=()):
            rows = rows.reshape(N_PLANE, n_line, capacity, rows.shape[-1])
            rows = after(rows, (done[-1:], then))
            rows = lax.all_to_all(rows, "ep", 0, 0, axis_index_groups=planes)
            done.append(rows)
            return rows

        def in_plane_rows(rows):
            return in_plane(rows).reshape(n_dev * capacity, rows.shape[-1])

        def sum_line(parts):
            return lax.psum_scatter(parts, "ep", axis_index_groups=lines)

        parts = []
        for x_part in x_line:
            send_x = dispatch(pos_line, gate_line, x_part, capacity, False)
            parts.append([in_plane_rows(rows) for rows in send_x])
        recv_x = [jnp.concatenate([p[g] for p in parts], axis=1) for g in range(loc_exp)]
        pre_gate, pre_up, hidden = [], [], []
        for g in range(loc_exp):
            pg = jnp.dot(recv_x[g], wg_loc[g], preferred_element_type=F32)
            pu = jnp.dot(recv_x[g], wu_loc[g], preferred_element_type=F32)
            pre_gate.append(pg)
            pre_up.append(pu)
            hidden.append((jax.nn.silu(pg) * pu).astype(BF16))

        y_sums, dots = [], 0.0
        send_o = [[jnp.dot(hidden[g], wd_loc[g, :, cols], preferred_element_type=F32).astype(BF16) for g in range(loc_exp)]
                  for cols in columns(Y_PIECES)]
        for i in range(Y_PIECES):
            back = []
            for g in range(loc_exp):
                then = send_o[i + 1][0] if g + 1 == loc_exp and i + 1 < Y_PIECES else ()
                back.append(in_plane(send_o[i][g], then))
            y_part, dot_part = combine(pos_line, gate_line, back[0], back[1], dy_line, i, capacity, True)
            y_sums.append(sum_line(y_part))
            dots += dot_part
        y_loc = jnp.concatenate(y_sums, axis=1).astype(BF16)

        send_d = dispatch(pos_line, gate_line, dy_line, capacity, True)
        recv_d = [in_plane_rows(rows) for rows in send_d]
        d_gate_rows, d_up_rows, dwg, dwu, dwd = [], [], [], [], []
        for g in range(loc_exp):
            dg_rows = recv_d[g]
            d_hidden = lax.dot_general(dg_rows, wd_loc[g], (((1,), (1,)), ((), ())), preferred_element_type=F32).astype(BF16).astype(F32)
            sig = jax.nn.sigmoid(pre_gate[g])
            d_pg = (d_hidden * pre_up[g] * sig * (1.0 + pre_gate[g] * (1.0 - sig))).astype(BF16)
            d_pu = (d_hidden * jax.nn.silu(pre_gate[g])).astype(BF16)
            d_gate_rows.append(d_pg)
            d_up_rows.append(d_pu)
            outer = (((0,), (0,)), ((), ()))
            dwd.append(lax.dot_general(hidden[g], dg_rows, outer, preferred_element_type=F32))
            dwg.append(lax.dot_general(recv_x[g], d_pg, outer, preferred_element_type=F32))
            dwu.append(lax.dot_general(recv_x[g], d_pu, outer, preferred_element_type=F32))

        def dx_rows(g, cols):
            rows = (lax.dot_general(d_gate_rows[g], wg_loc[g, cols], (((1,), (1,)), ((), ())), preferred_element_type=F32)
                    + lax.dot_general(d_up_rows[g], wu_loc[g, cols], (((1,), (1,)), ((), ())), preferred_element_type=F32))
            return rows.astype(BF16)

        dx_sums = []
        send_dx = [[dx_rows(g, cols) for g in range(loc_exp)] for cols in columns(DX_PIECES)]
        for i in range(DX_PIECES):
            back = []
            for g in range(loc_exp):
                then = send_dx[i + 1][0] if g + 1 == loc_exp and i + 1 < DX_PIECES else ()
                back.append(in_plane(send_dx[i][g], then))
            dx_part = combine(pos_line, gate_line, back[0], back[1], None, i, capacity, False)[0]
            dx_sums.append(sum_line(dx_part))

        a_pick = lax.all_to_all(after(dots, done[-1]), "ep", 0, 0, axis_index_groups=lines)
        a_pick = a_pick.transpose(0, 2, 1, 3).reshape(n_exp, tok)

        d_pick = (a_pick - jnp.sum(a_pick * gate, axis=0, keepdims=True)) / pick_sum
        d_prob = jnp.where(hot, d_pick, 0.0) + (AUX_COEF * n_exp * load_frac / n_total)[:, None]
        d_logit = (prob * (d_prob - jnp.sum(prob * d_prob, axis=0, keepdims=True))).astype(BF16)
        dx_router = lax.dot_general(d_logit, w_router, (((0,), (1,)), ((), ())), preferred_element_type=F32)
        dx_loc = (jnp.concatenate(dx_sums, axis=1) + dx_router).astype(BF16)

        dwr_part = lax.dot_general(x_loc, d_logit, (((0,), (1,)), ((), ())), preferred_element_type=F32)
        dwr_part = dwr_part.reshape(n_dev, dim // n_dev, n_exp)
        dwr_sum = jnp.sum(lax.all_to_all(dwr_part, "ep", 0, 0), axis=0)
        dw_router = lax.all_gather(dwr_sum, "ep", tiled=True)
        return y_loc, aux_loss, dx_loc, dw_router, jnp.stack(dwg), jnp.stack(dwu), jnp.stack(dwd)

    tok_spec = P("ep")
    return jax.shard_map(
        local_block,
        mesh=mesh,
        in_specs=(tok_spec, P(), tok_spec, tok_spec, tok_spec, tok_spec, tok_spec),
        out_specs=(tok_spec, P(), tok_spec, P(), tok_spec, tok_spec, tok_spec),
        check_vma=False,
    )
```
